32 devices in a mesh: groups: 2 (over y), seq: 4 (over z), head: 4 (over x, core).
Axes of the slice: x: 2, y: 2, z: 4, core: 2. Of those that a mesh axis runs over, the one named last changes fastest.
Arguments:
- residual: bfloat16 [1024, 2048], P(('groups', 'seq')), parts along dimension 0, may hold values from -6 to 6
- query_in: bfloat16 [1024, 2048], P(('groups', 'seq'), 'head'), parts along dimension 0, may hold values from -6 to 6
- key_in: bfloat16 [1024, 2048], P(('groups', 'seq'), 'head'), parts along dimension 0, may hold values from -6 to 6
- value_in: bfloat16 [1024, 4096], P(('groups', 'seq'), 'head'), parts along dimension 0, may hold values from -6 to 6
- gating_in: bfloat16 [1024, 4096], P(('groups', 'seq'), 'head'), parts along dimension 0, may hold values from -6 to 6
- beta_logit: float32 [1024, 32], P(('groups', 'seq'), 'head'), parts along dimension 0, may hold values from -12 to 2
- decay_logit: float32 [1024, 32], P(('groups', 'seq'), 'head'), parts along dimension 0, may hold values from -16 to 1
- seq_length: int32 [2], P('groups'), parts along dimension 0, may hold values from 256 to 512
- conv_query: float32 [4, 2048], P(None, 'head'), may hold values from -3 to 3
- conv_key: float32 [4, 2048], P(None, 'head'), may hold values from -3 to 3
- conv_value: float32 [4, 4096], P(None, 'head'), may hold values from -3 to 3
- decay_rate: float32 [32], P('head'), may hold values from 0.5 to 17
- norm_gain: float32 [128], replicated, may hold values from 0.1 to 1.9
- out_weight: bfloat16 [4096, 2048], P('head'), may hold values from -0.09375 to 0.09375
- attn_gain: float32 [2048], replicated, may hold values from 0.1 to 1.9
- query_weight: bfloat16 [2048, 8192], P('seq', 'head'), may hold values from -1 to 1
- key_value_weight: bfloat16 [2048, 1024], P('seq'), may hold values from -10 to 10
Outputs:
- hidden_out: bfloat16 [1024, 2048], P(('groups', 'seq')), parts along dimension 0
- attention_out: bfloat16 [1024, 4096], P(('groups', 'seq'), 'head'), parts along dimension 0
The draws below stay inside these ranges and needn't reach their ends.
There are 2 independent parts, one for each index of `groups`. The reference program is written for one: setup_inputs(seed, part) draws one part's arguments, and reference() takes and returns one part's arrays. A program takes and returns all parts, laid end to end along the dimension named above; an argument that names none is the same for every part. Nothing has to cross between parts.
All inputs are finite; a program needn't handle non-finite values.
Results may differ from the reference program's by a relative error of at most 0.02.
The reference program's roundings to bfloat16 on the way count: a program that leaves them out, or rounds other values in their place, can miss the bound.
Values may be sent and summed in bfloat16 or wider, within the bound.
A program may use at most 128 MiB of HBM per device.

```python
import math
import jax
import jax.numpy as jnp
from jax import lax

MODEL_WIDTH = 2048
HK = 16
HV = 32
DK = 128
DV = 128
QUERY_HEADS = 16
KEY_VALUE_HEADS = 2
HEAD_WIDTH = 256
CONV = 4
TOK_DEV = 128
SEQUENCE_LENGTH = 512


def weight_pair(key):
    bound = 6.0 / math.sqrt(MODEL_WIDTH)
    first_matrix = jax.random.normal(jax.random.fold_in(key, 11), (MODEL_WIDTH, QUERY_HEADS * 2 * HEAD_WIDTH), jnp.float32) / math.sqrt(MODEL_WIDTH)
    first_matrix = jnp.clip(first_matrix, -bound, bound)
    second_matrix = jax.random.normal(jax.random.fold_in(key, 12), (MODEL_WIDTH, 2 * KEY_VALUE_HEADS * HEAD_WIDTH), jnp.float32) / math.sqrt(MODEL_WIDTH)
    second_matrix = jnp.clip(second_matrix, -bound, bound)
    return (first_matrix, second_matrix)


def draw_query_weight(key, part):
    return weight_pair(key)[0].astype(jnp.bfloat16)


def draw_key_value_weight(key, part):
    return weight_pair(key)[1].astype(jnp.bfloat16)


def draw_beta_logit(key, part):
    token_places = jnp.arange(SEQUENCE_LENGTH, dtype=jnp.int32)
    stretch_length = 3 * TOK_DEV
    stretch_total = SEQUENCE_LENGTH // stretch_length + 1
    quiet_table = jax.random.randint(jax.random.fold_in(key, 32), (stretch_total, HV), 0, 2)
    quiet_rows = quiet_table[token_places // stretch_length]
    active = jax.random.uniform(jax.random.fold_in(key, 31), (SEQUENCE_LENGTH, HV), jnp.float32, -2.5, 1.5)
    silent = jax.random.uniform(jax.random.fold_in(key, 33), (SEQUENCE_LENGTH, HV), jnp.float32, -12.0, -10.0)
    return jnp.where(quiet_rows == 1, silent, active)


def draw_decay_logit(key, part):
    token_places = jnp.arange(SEQUENCE_LENGTH, dtype=jnp.int32)
    slab_total = SEQUENCE_LENGTH // TOK_DEV
    slab_offset = jax.random.uniform(jax.random.fold_in(key, 24), (slab_total, HV), jnp.float32, -2.0, 1.0)
    starting_shift = -math.log(SEQUENCE_LENGTH) + jax.random.uniform(jax.random.fold_in(key, 21), (SEQUENCE_LENGTH, HV), jnp.float32, -1.5, 1.5)
    starting_shift = starting_shift + slab_offset[token_places // TOK_DEV]
    location_entries = jax.random.randint(jax.random.fold_in(key, 22), (3, HV), 0, SEQUENCE_LENGTH)
    contiguous_lines = jnp.any(token_places[:, None, None] == location_entries[None], axis=1)
    threshold_amount = jax.random.uniform(jax.random.fold_in(key, 23), (SEQUENCE_LENGTH, HV), jnp.float32, 0.0, 1.0)
    return jnp.where(contiguous_lines, threshold_amount, starting_shift)


def block_levels(own_key, shape, split, smallest, top_value):
    loudness = 1.0
    for dim, parts in split:
        draws = jax.random.uniform(jax.random.fold_in(jax.random.fold_in(own_key, 6), dim), (parts,), jnp.float32, smallest / len(split), top_value / len(split))
        loudness = loudness * jnp.repeat(jnp.exp(draws), shape[dim] // parts).reshape((-1,) + (1,) * (len(shape) - 1 - dim))
    return loudness


def gaussian(own_key, shape, deviation, most, shards=(), kind=jnp.bfloat16):
    result = jax.random.normal(own_key, shape, jnp.float32) * deviation
    if len(shards) > 0:
        result = block_levels(own_key, shape, shards, -0.22, 0.18) * result
    return jnp.clip(result, min=-most, max=most).astype(kind)


def setup_inputs(seed: int = 0, part: int = 0) -> dict:
    keys = jax.random.split(jax.random.key(seed), 18)
    own_keys = jax.random.split(jax.random.fold_in(keys[17], part), 18)
    return {
        "residual": gaussian(own_keys[0], (SEQUENCE_LENGTH, MODEL_WIDTH), 1.0, 6.0, ((0, 4),)),
        "query_in": gaussian(own_keys[1], (SEQUENCE_LENGTH, HK * DK), 1.0, 6.0, ((0, 4), (1, 4))),
        "key_in": gaussian(own_keys[2], (SEQUENCE_LENGTH, HK * DK), 1.0, 6.0, ((0, 4), (1, 4))),
        "value_in": gaussian(own_keys[3], (SEQUENCE_LENGTH, HV * DV), 1.0, 6.0, ((0, 4), (1, 4))),
        "gating_in": gaussian(own_keys[4], (SEQUENCE_LENGTH, HV * DV), 1.0, 6.0, ((0, 4), (1, 4))),
        "beta_logit": draw_beta_logit(jax.random.fold_in(jax.random.fold_in(keys[17], part), 71), part),
        "decay_logit": draw_decay_logit(jax.random.fold_in(jax.random.fold_in(keys[17], part), 71), part),
        "seq_length": jax.random.randint(own_keys[7], (1,), SEQUENCE_LENGTH // 2, SEQUENCE_LENGTH + 1).astype(jnp.int32),
        "conv_query": gaussian(keys[8], (CONV, HK * DK), 0.5, 3.0, ((1, 4),), jnp.float32),
        "conv_key": gaussian(keys[9], (CONV, HK * DK), 0.5, 3.0, ((1, 4),), jnp.float32),
        "conv_value": gaussian(keys[10], (CONV, HV * DV), 0.5, 3.0, ((1, 4),), jnp.float32),
        "decay_rate": jnp.clip(jnp.exp(math.log(17.0) - 3.5263605 * jax.random.uniform(keys[11], (HV,), jnp.float32) ** block_levels(keys[11], (HV,), ((0, 4),), -0.2, 0.2)), 0.5, 17.0),
        "norm_gain": jnp.clip(1.0 + 0.18 * jax.random.normal(keys[12], (DV,), jnp.float32), 0.1, 1.9),
        "out_weight": gaussian(keys[13], (HV * DV, MODEL_WIDTH), (HV * DV) ** -0.5, 0.09375, ((0, 4),)),
        "attn_gain": jnp.clip(1.0 + 0.18 * jax.random.normal(keys[14], (MODEL_WIDTH,), jnp.float32), 0.1, 1.9),
        "query_weight": draw_query_weight(jax.random.fold_in(keys[17], 71), part),
        "key_value_weight": draw_key_value_weight(jax.random.fold_in(keys[17], 71), part),
    }


EPSILON = 1e-06
NEGATIVE = -1e+30

def causal_conv(inputs, kernel):
    widened = inputs.astype(jnp.float32)
    padded = jnp.concatenate([jnp.zeros((CONV - 1, widened.shape[1]), jnp.float32), widened], 0)
    summed = jnp.zeros_like(widened)
    for offset in range(CONV):
        summed = summed + kernel[offset] * padded[offset:offset + widened.shape[0]]
    return jax.nn.silu(summed)

def unit_rows(tensor):
    return tensor / jnp.sqrt(lax.optimization_barrier(jnp.sum(tensor * tensor, -1, keepdims=True)) + EPSILON)

def reference(residual, query_in, key_in, value_in, gating_in, beta_logit, decay_logit, seq_length, conv_query, conv_key, conv_value, decay_rate, norm_gain, out_weight, attn_gain, query_weight, key_value_weight):
    highest_index = lax.Precision.HIGHEST
    positions = jnp.arange(SEQUENCE_LENGTH, dtype=jnp.int32)
    length_now = seq_length[0].astype(jnp.int32)
    alive_mask = (positions < length_now).astype(jnp.float32)
    queries = unit_rows(causal_conv(query_in, conv_query).reshape(SEQUENCE_LENGTH, HK, DK)) * DK ** (-0.5)
    keyset = unit_rows(causal_conv(key_in, conv_key).reshape(SEQUENCE_LENGTH, HK, DK))
    values = causal_conv(value_in, conv_value).reshape(SEQUENCE_LENGTH, HV, DV)
    queries = jnp.repeat(queries, HV // HK, axis=1)
    keyset = jnp.repeat(keyset, HV // HK, axis=1)
    betas = jax.nn.sigmoid(beta_logit) * alive_mask[:, None]
    log_decay = -decay_rate[None, :] * jax.nn.softplus(decay_logit) * alive_mask[:, None]

    def advance(recurrent_state, inputs):
        current_query, current_key, value_now, beta_now, decay_now = inputs
        recurrent_state = jnp.exp(decay_now)[:, None, None] * recurrent_state
        prediction = jnp.einsum('ino,in->io', recurrent_state, current_key, precision=highest_index)
        recurrent_state = recurrent_state + beta_now[:, None, None] * current_key[:, :, None] * (value_now - prediction)[:, None, :]
        return (recurrent_state, jnp.einsum('ino,in->io', recurrent_state, current_query, precision=highest_index))
    initial = jnp.zeros((HV, DK, DV), jnp.float32)
    _, outputs = lax.scan(advance, initial, (queries, keyset, values, betas, log_decay))
    gating = gating_in.astype(jnp.float32).reshape(SEQUENCE_LENGTH, HV, DV)
    scaled = outputs * lax.rsqrt(lax.optimization_barrier(jnp.mean(outputs * outputs, -1, keepdims=True)) + EPSILON)
    gated = (scaled * norm_gain * jax.nn.silu(gating)).astype(jnp.bfloat16).reshape(SEQUENCE_LENGTH, HV * DV)
    summed = jnp.dot(gated, out_weight, preferred_element_type=jnp.float32)
    hidden_out = (residual.astype(jnp.float32) + summed).astype(jnp.bfloat16)
    widened = hidden_out.astype(jnp.float32)
    normalized = (widened * lax.rsqrt(lax.optimization_barrier(jnp.mean(widened * widened, -1, keepdims=True)) + EPSILON) * attn_gain).astype(jnp.bfloat16)
    projected = jnp.dot(normalized, query_weight, preferred_element_type=jnp.float32).reshape(SEQUENCE_LENGTH, QUERY_HEADS, 2, HEAD_WIDTH)
    queries_att = projected[:, :, 0].astype(jnp.bfloat16)
    gating_att = projected[:, :, 1]
    key_value_full = jnp.dot(normalized, key_value_weight, preferred_element_type=jnp.float32).reshape(SEQUENCE_LENGTH, 2, KEY_VALUE_HEADS, HEAD_WIDTH).astype(jnp.bfloat16)
    group_width = QUERY_HEADS // KEY_VALUE_HEADS
    key_heads = jnp.repeat(key_value_full[:, 0].transpose(1, 0, 2), group_width, 0)
    value_heads = jnp.repeat(key_value_full[:, 1].transpose(1, 0, 2), group_width, 0)
    visible = (positions[None, :] <= positions[:, None]) & (positions[None, :] < length_now)

    def attend_head(operands):
        head_query, head_key, head_value = operands
        scores = jnp.dot(head_query, head_key.T, preferred_element_type=jnp.float32) * HEAD_WIDTH ** (-0.5)
        scores = jnp.where(visible, scores, NEGATIVE)
        peak = lax.optimization_barrier(jnp.max(scores, -1, keepdims=True))
        weights = jnp.where(visible, jnp.exp(scores - peak), 0.0)
        denominator = lax.optimization_barrier(jnp.sum(weights, -1, keepdims=True))
        return jnp.dot(weights.astype(jnp.bfloat16), head_value, preferred_element_type=jnp.float32) / denominator
    attended = lax.map(attend_head, (queries_att.transpose(1, 0, 2), key_heads, value_heads))
    attention_out = (attended.transpose(1, 0, 2) * jax.nn.sigmoid(gating_att)).astype(jnp.bfloat16).reshape(SEQUENCE_LENGTH, QUERY_HEADS * HEAD_WIDTH)
    return (hidden_out, attention_out)
```

```python
import functools

import jax
import jax.numpy as jnp
from jax import lax
from jax.experimental import pallas as pl
from jax.experimental.pallas import tpu as pltpu
from jax.sharding import PartitionSpec as P

DK = 128
DV = 128
QUERY_HEADS = 16
KEY_VALUE_HEADS = 2
HEAD_WIDTH = 256
CONV = 4
PAD = 8

EPSILON = 1e-06
NEGATIVE = -1e30
MESH = pl.DeviceIdType.MESH
HIGHEST = lax.Precision.HIGHEST


def mm(a, b, contract=((1,), (0,))):
    return lax.dot_general(
        a, b, (contract, ((), ())), precision=HIGHEST, preferred_element_type=jnp.float32
    )


def delta_kernel(
    count,
    q_ref,
    k_ref,
    v_ref,
    gate_ref,
    tail_ref,
    beta_ref,
    decay_ref,
    decay_t_ref,
    length_ref,
    cq_ref,
    ck_ref,
    cv_ref,
    rate_ref,
    rate_t_ref,
    gain_ref,
    out_ref,
    joined,
    enter,
    leave,
    send_sems,
    recv_sems,
):
    me = lax.axis_index("seq")
    rows = q_ref.shape[0]
    key_heads = q_ref.shape[1] // DK
    value_heads = v_ref.shape[1] // DV
    share = value_heads // key_heads
    barrier = pltpu.get_barrier_semaphore()

    for peer in (lax.rem(me + 1, count), lax.rem(me + count - 1, count)):
        pl.semaphore_signal(barrier, inc=1, device_id={"seq": peer}, device_id_type=MESH)
    pl.semaphore_wait(barrier, 2)

    @pl.when(me == 0)
    def _():
        enter[...] = jnp.zeros_like(enter)

    q_width = key_heads * DK
    joined[:PAD] = tail_ref[...]
    joined[PAD:, :q_width] = q_ref[...].astype(jnp.float32)
    joined[PAD:, q_width : 2 * q_width] = k_ref[...].astype(jnp.float32)
    joined[PAD:, 2 * q_width :] = v_ref[...].astype(jnp.float32)

    def conv(base, taps, h):
        column = base + h * DK
        total = jnp.zeros((rows, DK), jnp.float32)
        for j in range(CONV):
            first = PAD - CONV + 1 + j
            total = total + taps[j : j + 1, h * DK : (h + 1) * DK] * joined[
                first : first + rows, column : column + DK
            ]
        return total * jax.nn.sigmoid(total)

    def unit(x):
        return x / jnp.sqrt(jnp.sum(x * x, -1, keepdims=True) + EPSILON)

    length = length_ref[0]
    start = me * rows
    at_row = start + lax.broadcasted_iota(jnp.int32, (rows, value_heads), 0)
    alive = (at_row < length).astype(jnp.float32)
    at_column = start + lax.broadcasted_iota(jnp.int32, (value_heads, rows), 1)
    alive_t = (at_column < length).astype(jnp.float32)

    def softplus(x):
        return jnp.maximum(x, 0.0) + jnp.log1p(jnp.exp(-jnp.abs(x)))

    beta = jax.nn.sigmoid(beta_ref[...]) * alive
    step = -rate_ref[...] * softplus(decay_ref[...]) * alive
    step_t = -rate_t_ref[...] * softplus(decay_t_ref[...]) * alive_t
    row = lax.broadcasted_iota(jnp.int32, (rows, rows), 0)
    column = lax.broadcasted_iota(jnp.int32, (rows, rows), 1)
    inclusive = row >= column
    run = mm(inclusive.astype(jnp.float32), step)
    run_t = mm(step_t, (row <= column).astype(jnp.float32))
    growth = jnp.exp(run)
    ending = jnp.exp(run[rows - 1 : rows] - run)
    eye = (row == column).astype(jnp.float32)

    queries, keyset, grams, mixes = [], [], [], []
    for g in range(key_heads):
        q = unit(conv(0, cq_ref, g)) * DK ** (-0.5)
        k = unit(conv(q_width, ck_ref, g))
        queries.append(q)
        keyset.append(k)
        grams.append(mm(k, k, ((1,), (1,))))
        mixes.append(mm(q, k, ((1,), (1,))))

    within, lower, inverse = [], [], []
    for h in range(value_heads):
        spread = run[:, h : h + 1] - run_t[h : h + 1, :]
        w = jnp.where(inclusive, jnp.exp(jnp.where(inclusive, spread, 0.0)), 0.0)
        within.append(w)
        low = jnp.where(row > column, beta[:, h : h + 1] * w * grams[h // share], 0.0)
        lower.append(low)
        pair = (row // 2 == column // 2) & (row > column)
        inverse.append(eye - jnp.where(pair, low, 0.0))
    size = 2
    while size < rows:
        off = (row // (2 * size) == column // (2 * size)) & (row // size > column // size)
        half = [mm(jnp.where(off, low, 0.0), x) for low, x in zip(lower, inverse)]
        inverse = [x - mm(x, y) for x, y in zip(inverse, half)]
        size *= 2

    local, carry, transition, injected = [], [], [], []
    for h in range(value_heads):
        k = keyset[h // share]
        v = conv(2 * q_width, cv_ref, h)
        b = beta[:, h : h + 1]
        w = mm(inverse[h], b * growth[:, h : h + 1] * k)
        u = mm(inverse[h], b * v)
        mix = mixes[h // share] * within[h]
        stop = ending[:, h : h + 1] * k
        local.append(mm(mix, u))
        carry.append(growth[:, h : h + 1] * queries[h // share] - mm(mix, w))
        transition.append(
            growth[rows - 1 : rows, h : h + 1] * eye - mm(stop, w, ((0,), (0,)))
        )
        injected.append(mm(stop, u, ((0,), (0,))))

    copies = []
    for h in range(value_heads):
        copy = pltpu.make_async_remote_copy(
            src_ref=leave.at[h],
            dst_ref=enter.at[h],
            send_sem=send_sems.at[h],
            recv_sem=recv_sems.at[h],
            device_id={"seq": lax.rem(me + 1, count)},
            device_id_type=MESH,
        )
        copies.append(copy)

        @pl.when(me > 0)
        def _():
            copy.wait_recv()

        state = enter[h]
        leave[h] = mm(transition[h], state) + injected[h]
        o = local[h] + mm(carry[h], state)
        scaled = o * lax.rsqrt(jnp.mean(o * o, -1, keepdims=True) + EPSILON) * gain_ref[...]
        gate = gate_ref[:, h * DV : (h + 1) * DV].astype(jnp.float32)
        out_ref[:, h * DV : (h + 1) * DV] = (
            scaled * (gate * jax.nn.sigmoid(gate))
        ).astype(out_ref.dtype)

        @pl.when(me < count - 1)
        def _():
            copy.start()

    @pl.when(me < count - 1)
    def _():
        for copy in copies:
            copy.wait_send()


def delta(count, q, k, v, gate, beta_logit, decay_logit, seq_length, cq, ck, cv, rate, gain):
    rows, value_heads = beta_logit.shape
    width = q.shape[1] + k.shape[1] + v.shape[1]
    rim = rows - CONV + 1
    tail = jnp.concatenate([q[rim:], k[rim:], v[rim:]], 1)
    tail = shifted(tail, "seq", 1).astype(jnp.float32)
    tail = jnp.concatenate([jnp.zeros((PAD - CONV + 1, width), jnp.float32), tail], 0)
    vmem = pl.BlockSpec(memory_space=pltpu.VMEM)
    smem = pl.BlockSpec(memory_space=pltpu.SMEM)
    return pl.pallas_call(
        functools.partial(delta_kernel, count),
        out_shape=jax.ShapeDtypeStruct(gate.shape, jnp.bfloat16),
        in_specs=[vmem] * 8 + [smem] + [vmem] * 6,
        out_specs=vmem,
        scratch_shapes=[
            pltpu.VMEM((rows + PAD, width), jnp.float32),
            pltpu.VMEM((value_heads, DK, DV), jnp.float32),
            pltpu.VMEM((value_heads, DK, DV), jnp.float32),
            pltpu.SemaphoreType.DMA((value_heads,)),
            pltpu.SemaphoreType.DMA((value_heads,)),
        ],
        compiler_params=pltpu.CompilerParams(
            collective_id=0, has_side_effects=True, vmem_limit_bytes=32 * 2**20
        ),
        cost_estimate=pl.CostEstimate(
            flops=50_000_000_000, bytes_accessed=4_000_000, transcendentals=0
        ),
        name="delta_rule",
    )(
        q,
        k,
        v,
        gate,
        tail,
        beta_logit,
        decay_logit,
        decay_logit.T,
        seq_length,
        cq,
        ck,
        cv,
        rate[None, :],
        rate[:, None],
        gain[None, :],
    )


def shifted(shard, axis, by):
    count = lax.axis_size(axis)
    pairs = [(i, i + by) for i in range(count) if 0 <= i + by < count]
    return lax.ppermute(shard, axis, pairs)


def rms_scaled(tensor, gain_vector):
    return tensor * lax.rsqrt(jnp.mean(tensor * tensor, -1, keepdims=True) + EPSILON) * gain_vector


def pick(key_value_weight, query_weight):
    attention_channel_id = lax.axis_index("head")
    query_head_rows = query_weight.shape[1] // (2 * HEAD_WIDTH)
    key_value_head = attention_channel_id * query_head_rows // (QUERY_HEADS // KEY_VALUE_HEADS)
    key_start = key_value_head * HEAD_WIDTH
    value_offset = (KEY_VALUE_HEADS + key_value_head) * HEAD_WIDTH
    return jnp.concatenate(
        [
            lax.dynamic_slice_in_dim(key_value_weight, key_start, HEAD_WIDTH, 1),
            lax.dynamic_slice_in_dim(key_value_weight, value_offset, HEAD_WIDTH, 1),
        ],
        1,
    )


def shards(
    residual,
    query_in,
    key_in,
    value_in,
    gating_in,
    beta_logit,
    decay_logit,
    seq_length,
    conv_query,
    conv_key,
    conv_value,
    decay_rate,
    norm_gain,
    out_weight,
    attn_gain,
    query_weight,
    key_value_weight,
):
    row_count = residual.shape[0]
    seq_rank = lax.axis_index("seq")
    positions = seq_rank * row_count + jnp.arange(row_count, dtype=jnp.int32)
    length_now = seq_length[0]
    all_query_weight = lax.all_gather(query_weight, "seq", axis=0, tiled=True)
    picked = pick(key_value_weight, query_weight)
    all_picked = lax.all_gather(picked, "seq", axis=0, tiled=True)
    gated = delta(
        lax.axis_size("seq"),
        query_in,
        key_in,
        value_in,
        gating_in,
        beta_logit,
        decay_logit,
        seq_length,
        conv_query,
        conv_key,
        conv_value,
        decay_rate,
        norm_gain,
    )
    summed = lax.psum(jnp.dot(gated, out_weight, preferred_element_type=jnp.float32), "head")
    hidden_out = (residual.astype(jnp.float32) + summed).astype(jnp.bfloat16)
    normalized = rms_scaled(hidden_out.astype(jnp.float32), attn_gain).astype(jnp.bfloat16)
    query_head_rows = query_weight.shape[1] // (2 * HEAD_WIDTH)
    query_proj = jnp.dot(
        normalized,
        all_query_weight,
        preferred_element_type=jnp.float32,
    )
    kv_proj = jnp.dot(
        normalized,
        all_picked,
        preferred_element_type=jnp.float32,
    )
    query_proj = query_proj.reshape(row_count, query_head_rows, 2, HEAD_WIDTH)
    queries_att = query_proj[:, :, 0].astype(jnp.bfloat16)
    gating_att = query_proj[:, :, 1]
    half_rows = row_count // 2
    blocks = (queries_att[:half_rows], queries_att[half_rows:])
    block_positions = (positions[:half_rows], positions[half_rows:])
    start_state = (
        jnp.full((query_head_rows, half_rows), NEGATIVE, jnp.float32),
        jnp.zeros((query_head_rows, half_rows), jnp.float32),
        jnp.zeros((query_head_rows, half_rows, HEAD_WIDTH), jnp.float32),
    )
    running = (start_state, start_state)
    offset = jnp.int32(0)
    both = lax.all_gather(kv_proj.astype(jnp.bfloat16), "seq", axis=0, tiled=True)
    key_piece = both[:, :HEAD_WIDTH]
    value_piece = both[:, HEAD_WIDTH:]
    key_positions = jnp.arange(key_piece.shape[0], dtype=jnp.int32)
    updated = []
    for block_index in range(2):
        block_queries = blocks[block_index]
        query_positions = block_positions[block_index]
        needed = jnp.logical_and(offset <= query_positions[-1], offset < length_now)

        def refresh(recurrent_state):
            peak, _, _ = recurrent_state
            scores = jnp.einsum(
                "qhd,kd->hqk", block_queries, key_piece, preferred_element_type=jnp.float32
            ) * HEAD_WIDTH ** (-0.5)
            visible = (key_positions[None, :] <= query_positions[:, None]) & (
                key_positions[None, :] < length_now
            )
            scores = jnp.where(visible[None], scores, NEGATIVE)
            new_peak = jnp.maximum(peak, jnp.max(scores, -1))
            weights = jnp.where(visible[None], jnp.exp(scores - new_peak[..., None]), 0.0)
            return (
                new_peak,
                jnp.sum(weights, -1),
                jnp.einsum(
                    "hqk,kd->hqd",
                    weights.astype(jnp.bfloat16),
                    value_piece,
                    preferred_element_type=jnp.float32,
                ),
            )

        updated.append(
            lax.cond(needed, refresh, lambda recurrent_state: recurrent_state, running[block_index])
        )
    finished = tuple(updated)
    results = [
        (recurrent_state[2] / recurrent_state[1][..., None]).transpose(1, 0, 2)
        for recurrent_state in finished
    ]
    attended = jnp.concatenate(results, 0)
    attention_out = (
        (attended * jax.nn.sigmoid(gating_att))
        .astype(jnp.bfloat16)
        .reshape(row_count, query_head_rows * HEAD_WIDTH)
    )
    return (hidden_out, attention_out)


def solution(mesh):
    placed = (
        P(("groups", "seq"), None),
        P(("groups", "seq"), "head"),
        P(("groups", "seq"), "head"),
        P(("groups", "seq"), "head"),
        P(("groups", "seq"), "head"),
        P(("groups", "seq"), "head"),
        P(("groups", "seq"), "head"),
        P("groups"),
        P(None, "head"),
        P(None, "head"),
        P(None, "head"),
        P("head"),
        P(),
        P("head", None),
        P(),
        P("seq", "head"),
        P("seq", None),
    )

    return jax.shard_map(
        shards,
        mesh=mesh,
        in_specs=placed,
        out_specs=(P(("groups", "seq"), None), P(("groups", "seq"), "head")),
        check_vma=False,
    )
```

```python
import functools

import jax
import jax.numpy as jnp
from jax import lax
from jax.experimental import pallas as pl
from jax.experimental.pallas import tpu as pltpu
from jax.sharding import PartitionSpec as P

DK = 128
DV = 128
QUERY_HEADS = 16
KEY_VALUE_HEADS = 2
HEAD_WIDTH = 256
CONV = 4
PAD = 8

EPSILON = 1e-06
NEGATIVE = -1e30
MESH = pl.DeviceIdType.MESH
HIGHEST = lax.Precision.HIGHEST


def mm(a, b, contract=((1,), (0,))):
    return lax.dot_general(
        a, b, (contract, ((), ())), precision=HIGHEST, preferred_element_type=jnp.float32
    )


def delta_kernel(
    count,
    groups,
    q_ref,
    k_ref,
    v_ref,
    gate_ref,
    tail_ref,
    beta_ref,
    decay_ref,
    decay_t_ref,
    length_ref,
    cq_ref,
    ck_ref,
    cv_ref,
    rate_ref,
    rate_t_ref,
    gain_ref,
    w_ref,
    out_ref,
    full_ref,
    joined,
    enter,
    leave,
    send_sems,
    recv_sems,
    own_sem,
    z_send,
    z_recv,
    y_send,
    y_recv,
):
    me = lax.axis_index("seq")
    rows = q_ref.shape[0]
    key_heads = q_ref.shape[1] // DK
    value_heads = v_ref.shape[1] // DV
    share = value_heads // key_heads
    barrier = pltpu.get_barrier_semaphore()

    for peer in (lax.rem(me + 1, count), lax.rem(me + count - 1, count)):
        pl.semaphore_signal(barrier, inc=1, device_id={"seq": peer}, device_id_type=MESH)
    part = lax.axis_index("groups")
    for e in range(1, groups):
        pl.semaphore_signal(
            barrier,
            inc=1,
            device_id={"groups": lax.rem(part + e, groups)},
            device_id_type=MESH,
        )
    pl.semaphore_wait(barrier, 1 + groups)

    depth = w_ref.shape[0]
    piece = depth // groups

    def rows_of(block, which):
        return full_ref.at[pl.ds(pl.multiple_of(block * depth + which * piece, piece), piece)]

    def inside(block):
        return (block >= 0) & (block < count)

    def clamp(block):
        return jnp.clip(block, 0, count - 1)

    def along(d, j):
        sign = 1 if d == 0 else -1
        block = clamp(me - sign * j)
        source = w_ref.at[pl.ds(pl.multiple_of(part * piece, piece), piece)]
        return pltpu.make_async_remote_copy(
            src_ref=source if j == 0 else rows_of(block, part),
            dst_ref=rows_of(block, part),
            send_sem=z_send.at[d, j],
            recv_sem=z_recv.at[d, j],
            device_id={"seq": clamp(me + sign)},
            device_id_type=MESH,
        ), inside(me - sign * j) & inside(me + sign)

    def landing(d, j):
        sign = 1 if d == 0 else -1
        block = clamp(me - sign * (j + 1))
        return pltpu.make_async_remote_copy(
            src_ref=rows_of(block, part),
            dst_ref=rows_of(block, part),
            send_sem=z_send.at[d, j],
            recv_sem=z_recv.at[d, j],
            device_id={"seq": clamp(me + sign)},
            device_id_type=MESH,
        ), inside(me - sign * (j + 1))

    def across(e, d, j, which):
        sign = 1 if d == 0 else -1
        block = clamp(me - sign * (j + 1))
        return pltpu.make_async_remote_copy(
            src_ref=rows_of(block, which),
            dst_ref=rows_of(block, which),
            send_sem=y_send.at[e - 1, d, j],
            recv_sem=y_recv.at[e - 1, d, j],
            device_id={"groups": lax.rem(part + e, groups)},
            device_id_type=MESH,
        )

    def relay(j):
        for d in range(2):
            copy, here = landing(d, j)

            @pl.when(here)
            def _():
                copy.wait_recv()
                for e in range(1, groups):
                    across(e, d, j, part).start()

            if j + 1 < count - 1:
                onward, go = along(d, j + 1)
                pl.when(go)(onward.start)

    own = pltpu.make_async_copy(
        w_ref, full_ref.at[pl.ds(pl.multiple_of(me * depth, depth), depth)], own_sem
    )
    for d in range(2):
        first_copy, go = along(d, 0)
        pl.when(go)(first_copy.start)
    own.start()

    @pl.when(me == 0)
    def _():
        enter[...] = jnp.zeros_like(enter)

    q_width = key_heads * DK
    joined[:PAD] = tail_ref[...]
    joined[PAD:, :q_width] = q_ref[...].astype(jnp.float32)
    joined[PAD:, q_width : 2 * q_width] = k_ref[...].astype(jnp.float32)
    joined[PAD:, 2 * q_width :] = v_ref[...].astype(jnp.float32)

    def conv(base, taps, h):
        column = base + h * DK
        total = jnp.zeros((rows, DK), jnp.float32)
        for j in range(CONV):
            first = PAD - CONV + 1 + j
            total = total + taps[j : j + 1, h * DK : (h + 1) * DK] * joined[
                first : first + rows, column : column + DK
            ]
        return total * jax.nn.sigmoid(total)

    def unit(x):
        return x / jnp.sqrt(jnp.sum(x * x, -1, keepdims=True) + EPSILON)

    length = length_ref[0]
    start = me * rows
    at_row = start + lax.broadcasted_iota(jnp.int32, (rows, value_heads), 0)
    alive = (at_row < length).astype(jnp.float32)
    at_column = start + lax.broadcasted_iota(jnp.int32, (value_heads, rows), 1)
    alive_t = (at_column < length).astype(jnp.float32)

    def softplus(x):
        return jnp.maximum(x, 0.0) + jnp.log1p(jnp.exp(-jnp.abs(x)))

    beta = jax.nn.sigmoid(beta_ref[...]) * alive
    step = -rate_ref[...] * softplus(decay_ref[...]) * alive
    step_t = -rate_t_ref[...] * softplus(decay_t_ref[...]) * alive_t
    row = lax.broadcasted_iota(jnp.int32, (rows, rows), 0)
    column = lax.broadcasted_iota(jnp.int32, (rows, rows), 1)
    inclusive = row >= column
    run = mm(inclusive.astype(jnp.float32), step)
    run_t = mm(step_t, (row <= column).astype(jnp.float32))
    growth = jnp.exp(run)
    ending = jnp.exp(run[rows - 1 : rows] - run)
    eye = (row == column).astype(jnp.float32)

    queries, keyset, grams, mixes = [], [], [], []
    for g in range(key_heads):
        q = unit(conv(0, cq_ref, g)) * DK ** (-0.5)
        k = unit(conv(q_width, ck_ref, g))
        queries.append(q)
        keyset.append(k)
        grams.append(mm(k, k, ((1,), (1,))))
        mixes.append(mm(q, k, ((1,), (1,))))

    within, lower, inverse = [], [], []
    for h in range(value_heads):
        spread = run[:, h : h + 1] - run_t[h : h + 1, :]
        w = jnp.where(inclusive, jnp.exp(jnp.where(inclusive, spread, 0.0)), 0.0)
        within.append(w)
        low = jnp.where(row > column, beta[:, h : h + 1] * w * grams[h // share], 0.0)
        lower.append(low)
        pair = (row // 2 == column // 2) & (row > column)
        inverse.append(eye - jnp.where(pair, low, 0.0))
    size = 2
    while size < rows:
        off = (row // (2 * size) == column // (2 * size)) & (row // size > column // size)
        half = [mm(jnp.where(off, low, 0.0), x) for low, x in zip(lower, inverse)]
        inverse = [x - mm(x, y) for x, y in zip(inverse, half)]
        size *= 2

    local, carry, transition, injected = [], [], [], []
    for h in range(value_heads):
        k = keyset[h // share]
        v = conv(2 * q_width, cv_ref, h)
        b = beta[:, h : h + 1]
        w = mm(inverse[h], b * growth[:, h : h + 1] * k)
        u = mm(inverse[h], b * v)
        mix = mixes[h // share] * within[h]
        stop = ending[:, h : h + 1] * k
        local.append(mm(mix, u))
        carry.append(growth[:, h : h + 1] * queries[h // share] - mm(mix, w))
        transition.append(
            growth[rows - 1 : rows, h : h + 1] * eye - mm(stop, w, ((0,), (0,)))
        )
        injected.append(mm(stop, u, ((0,), (0,))))

    relay(0)
    copies = []
    for h in range(value_heads):
        copy = pltpu.make_async_remote_copy(
            src_ref=leave.at[h],
            dst_ref=enter.at[h],
            send_sem=send_sems.at[h],
            recv_sem=recv_sems.at[h],
            device_id={"seq": lax.rem(me + 1, count)},
            device_id_type=MESH,
        )
        copies.append(copy)

        @pl.when(me > 0)
        def _():
            copy.wait_recv()

        state = enter[h]
        leave[h] = mm(transition[h], state) + injected[h]
        o = local[h] + mm(carry[h], state)
        scaled = o * lax.rsqrt(jnp.mean(o * o, -1, keepdims=True) + EPSILON) * gain_ref[...]
        gate = gate_ref[:, h * DV : (h + 1) * DV].astype(jnp.float32)
        out_ref[:, h * DV : (h + 1) * DV] = (
            scaled * (gate * jax.nn.sigmoid(gate))
        ).astype(out_ref.dtype)

        @pl.when(me < count - 1)
        def _():
            copy.start()

    @pl.when(me < count - 1)
    def _():
        for copy in copies:
            copy.wait_send()

    for j in range(1, count - 1):
        relay(j)
    own.wait()
    for j in range(count - 1):
        for d in range(2):
            sent, go = along(d, j)
            pl.when(go)(sent.wait_send)
            _, here = landing(d, j)

            @pl.when(here)
            def _():
                for e in range(1, groups):
                    across(e, d, j, part).wait_send()
                    across(e, d, j, lax.rem(part + groups - e, groups)).wait_recv()


def delta(count, weights, q, k, v, gate, beta_logit, decay_logit, seq_length, cq, ck, cv, rate, gain):
    rows, value_heads = beta_logit.shape
    width = q.shape[1] + k.shape[1] + v.shape[1]
    rim = rows - CONV + 1
    groups = lax.axis_size("groups")
    tail = jnp.concatenate([q[rim:], k[rim:], v[rim:]], 1)
    tail = shifted(tail, "seq", 1).astype(jnp.float32)
    tail = jnp.concatenate([jnp.zeros((PAD - CONV + 1, width), jnp.float32), tail], 0)
    vmem = pl.BlockSpec(memory_space=pltpu.VMEM)
    smem = pl.BlockSpec(memory_space=pltpu.SMEM)
    return pl.pallas_call(
        functools.partial(delta_kernel, count, groups),
        out_shape=(
            jax.ShapeDtypeStruct(gate.shape, jnp.bfloat16),
            jax.ShapeDtypeStruct((count * weights.shape[0], weights.shape[1]), jnp.bfloat16),
        ),
        in_specs=[vmem] * 8 + [smem] + [vmem] * 7,
        out_specs=(vmem, pl.BlockSpec(memory_space=pl.ANY)),
        scratch_shapes=[
            pltpu.VMEM((rows + PAD, width), jnp.float32),
            pltpu.VMEM((value_heads, DK, DV), jnp.float32),
            pltpu.VMEM((value_heads, DK, DV), jnp.float32),
            pltpu.SemaphoreType.DMA((value_heads,)),
            pltpu.SemaphoreType.DMA((value_heads,)),
            pltpu.SemaphoreType.DMA,
            pltpu.SemaphoreType.DMA((2, count - 1)),
            pltpu.SemaphoreType.DMA((2, count - 1)),
            pltpu.SemaphoreType.DMA((groups - 1, 2, count - 1)),
            pltpu.SemaphoreType.DMA((groups - 1, 2, count - 1)),
        ],
        compiler_params=pltpu.CompilerParams(
            collective_id=0, has_side_effects=True, vmem_limit_bytes=32 * 2**20
        ),
        cost_estimate=pl.CostEstimate(
            flops=50_000_000_000, bytes_accessed=4_000_000, transcendentals=0
        ),
        name="delta_rule",
    )(
        q,
        k,
        v,
        gate,
        tail,
        beta_logit,
        decay_logit,
        decay_logit.T,
        seq_length,
        cq,
        ck,
        cv,
        rate[None, :],
        rate[:, None],
        gain[None, :],
        weights,
    )


def shifted(shard, axis, by):
    count = lax.axis_size(axis)
    pairs = [(i, i + by) for i in range(count) if 0 <= i + by < count]
    return lax.ppermute(shard, axis, pairs)


def rms_scaled(tensor, gain_vector):
    return tensor * lax.rsqrt(jnp.mean(tensor * tensor, -1, keepdims=True) + EPSILON) * gain_vector


def pick(key_value_weight, query_weight):
    attention_channel_id = lax.axis_index("head")
    query_head_rows = query_weight.shape[1] // (2 * HEAD_WIDTH)
    key_value_head = attention_channel_id * query_head_rows // (QUERY_HEADS // KEY_VALUE_HEADS)
    key_start = key_value_head * HEAD_WIDTH
    value_offset = (KEY_VALUE_HEADS + key_value_head) * HEAD_WIDTH
    return jnp.concatenate(
        [
            lax.dynamic_slice_in_dim(key_value_weight, key_start, HEAD_WIDTH, 1),
            lax.dynamic_slice_in_dim(key_value_weight, value_offset, HEAD_WIDTH, 1),
        ],
        1,
    )


def shards(
    residual,
    query_in,
    key_in,
    value_in,
    gating_in,
    beta_logit,
    decay_logit,
    seq_length,
    conv_query,
    conv_key,
    conv_value,
    decay_rate,
    norm_gain,
    out_weight,
    attn_gain,
    query_weight,
    key_value_weight,
):
    row_count = residual.shape[0]
    seq_rank = lax.axis_index("seq")
    positions = seq_rank * row_count + jnp.arange(row_count, dtype=jnp.int32)
    length_now = seq_length[0]
    weights = jnp.concatenate([query_weight, pick(key_value_weight, query_weight)], 1)
    gated, all_weights = delta(
        lax.axis_size("seq"),
        weights,
        query_in,
        key_in,
        value_in,
        gating_in,
        beta_logit,
        decay_logit,
        seq_length,
        conv_query,
        conv_key,
        conv_value,
        decay_rate,
        norm_gain,
    )
    summed = lax.psum(jnp.dot(gated, out_weight, preferred_element_type=jnp.float32), "head")
    hidden_out = (residual.astype(jnp.float32) + summed).astype(jnp.bfloat16)
    normalized = rms_scaled(hidden_out.astype(jnp.float32), attn_gain).astype(jnp.bfloat16)
    query_head_rows = query_weight.shape[1] // (2 * HEAD_WIDTH)
    projected = jnp.dot(normalized, all_weights, preferred_element_type=jnp.float32)
    query_proj = projected[:, : query_weight.shape[1]]
    kv_proj = projected[:, query_weight.shape[1] :]
    query_proj = query_proj.reshape(row_count, query_head_rows, 2, HEAD_WIDTH)
    queries_att = query_proj[:, :, 0].astype(jnp.bfloat16)
    gating_att = query_proj[:, :, 1]
    half_rows = row_count // 2
    blocks = (queries_att[:half_rows], queries_att[half_rows:])
    block_positions = (positions[:half_rows], positions[half_rows:])
    start_state = (
        jnp.full((query_head_rows, half_rows), NEGATIVE, jnp.float32),
        jnp.zeros((query_head_rows, half_rows), jnp.float32),
        jnp.zeros((query_head_rows, half_rows, HEAD_WIDTH), jnp.float32),
    )
    running = (start_state, start_state)
    offset = jnp.int32(0)
    both = lax.all_gather(kv_proj.astype(jnp.bfloat16), "seq", axis=0, tiled=True)
    key_piece = both[:, :HEAD_WIDTH]
    value_piece = both[:, HEAD_WIDTH:]
    key_positions = jnp.arange(key_piece.shape[0], dtype=jnp.int32)
    updated = []
    for block_index in range(2):
        block_queries = blocks[block_index]
        query_positions = block_positions[block_index]
        needed = jnp.logical_and(offset <= query_positions[-1], offset < length_now)

        def refresh(recurrent_state):
            peak, total, accum = recurrent_state
            scores = jnp.einsum(
                "qhd,kd->hqk", block_queries, key_piece, preferred_element_type=jnp.float32
            ) * HEAD_WIDTH ** (-0.5)
            visible = (key_positions[None, :] <= query_positions[:, None]) & (
                key_positions[None, :] < length_now
            )
            scores = jnp.where(visible[None], scores, NEGATIVE)
            new_peak = jnp.maximum(peak, jnp.max(scores, -1))
            weights = jnp.where(visible[None], jnp.exp(scores - new_peak[..., None]), 0.0)
            return (
                new_peak,
                jnp.sum(weights, -1),
                jnp.einsum(
                    "hqk,kd->hqd",
                    weights.astype(jnp.bfloat16),
                    value_piece,
                    preferred_element_type=jnp.float32,
                ),
            )

        updated.append(
            lax.cond(needed, refresh, lambda recurrent_state: recurrent_state, running[block_index])
        )
    finished = tuple(updated)
    results = [
        (recurrent_state[2] / recurrent_state[1][..., None]).transpose(1, 0, 2)
        for recurrent_state in finished
    ]
    attended = jnp.concatenate(results, 0)
    attention_out = (
        (attended * jax.nn.sigmoid(gating_att))
        .astype(jnp.bfloat16)
        .reshape(row_count, query_head_rows * HEAD_WIDTH)
    )
    return (hidden_out, attention_out)


def solution(mesh):
    placed = (
        P(("groups", "seq"), None),
        P(("groups", "seq"), "head"),
        P(("groups", "seq"), "head"),
        P(("groups", "seq"), "head"),
        P(("groups", "seq"), "head"),
        P(("groups", "seq"), "head"),
        P(("groups", "seq"), "head"),
        P("groups"),
        P(None, "head"),
        P(None, "head"),
        P(None, "head"),
        P("head"),
        P(),
        P("head", None),
        P(),
        P("seq", "head"),
        P("seq", None),
    )
    return jax.shard_map(
        shards,
        mesh=mesh,
        in_specs=placed,
        out_specs=(P(("groups", "seq"), None), P(("groups", "seq"), "head")),
        check_vma=False,
    )
```
